32 devices in a mesh: tile: 8 (over y, x, core), sub: 4 (over z).
Axes of the slice: x: 2, y: 2, z: 4, core: 2. Of those that a mesh axis runs over, the one named last changes fastest.
Arguments:
- pair_features: bfloat16 [8, 128, 128, 128], P('tile', 'sub'), may hold values from -6 to 6
- out_grad: bfloat16 [8, 128, 128, 128], P('tile', 'sub'), may hold values from -6 to 6
- bin_valid: int32 [640], replicated, may hold values 0 or 1
- first_kernel: bfloat16 [3, 3, 128, 128], replicated, may hold values from -0.1875 to 0.1875
- first_bias: float32 [128], replicated, may hold values from -3 to 3
- second_kernel: bfloat16 [3, 3, 128, 128], replicated, may hold values from -0.1875 to 0.1875
- second_bias: float32 [128], replicated, may hold values from -3 to 3
Outputs:
- block_out: bfloat16 [8, 128, 128, 128], P('tile', 'sub')
- feature_grad: bfloat16 [8, 128, 128, 128], P('tile', 'sub')
- kernel_one_grad: float32 [3, 3, 128, 128], replicated
- bias_one_grad: float32 [128], replicated
- kernel_two_grad: float32 [3, 3, 128, 128], replicated
- bias_two_grad: float32 [128], replicated
The draws below stay inside these ranges and needn't reach their ends.
Inputs may be any that keep to these rules, and one draw needn't show every extreme that they name: `bin_valid`: 1 marks a bin that passed filtering.
All inputs are finite; a program needn't handle non-finite values.
Results may differ from the reference program's by a relative error of at most 0.006.
Values may be sent and summed in bfloat16 or wider, within the bound.
No kernel may reach another device: no remote copies, remote signals or barrier semaphores. Data moves between devices by JAX's collectives and lax.ppermute only.
A program may use at most 128 MiB of HBM per device.

```python
import math
import jax
import jax.numpy as jnp
import numpy as np
from jax import lax

C = 128
TILE_BINS = 128
FIRST_DILATION = 8
SECOND_DILATION = 16
BAND_DIAGONALS = 4
TPG = 1
TILES = 8
TILE_ROWS = 2
COLS = 640
N_TILE = 8


def set_ends(entries, own_key, low, high):
    place = [jax.random.randint(jax.random.fold_in(own_key, axis), (), 0, length) for axis, length in enumerate(entries.shape)]
    widest = entries.shape.index(max(entries.shape))
    next_to = place[:widest] + [(place[widest] + 1) % entries.shape[widest]] + place[widest + 1:]
    return entries.at[tuple(place)].set(low).at[tuple(next_to)].set(high)


def shard_levels(rng, extent, pieces, low, largest):
    def one(position, blocks):
        draws = jax.random.uniform(jax.random.fold_in(jax.random.fold_in(rng, 6), position), (blocks,), jnp.float32, low / len(pieces), largest / len(pieces))
        return jnp.repeat(jnp.exp(draws), extent[position] // blocks).reshape((-1,) + (1,) * (len(extent) - position - 1))

    level = one(*pieces[0])
    for cut in pieces[1:]:
        level = level * one(*cut)
    return level


def gaussian(key, shape, scale, most, split=(), held_as=jnp.bfloat16):
    result = jax.random.normal(key, shape, jnp.float32) * scale
    if len(split) > 0:
        result = shard_levels(key, shape, split, -0.22, 0.18) * result
    return jnp.clip(result, min=-most, max=most).astype(held_as)


def setup_inputs(seed: int = 0) -> dict:
    streams_of = jax.random.split(jax.random.key(seed), 8)
    pair_features = gaussian(streams_of[0], (TILES, TILE_BINS, TILE_BINS, C), 1.0, 6.0, ((0, 8), (1, 4)))
    out_grad = gaussian(streams_of[1], (TILES, TILE_BINS, TILE_BINS, C), 1.0, 6.0, ((0, 8), (1, 4)))
    bin_valid = set_ends((jax.random.randint(streams_of[2], (COLS,), 0, 10) < 9).astype(jnp.int32), jax.random.fold_in(streams_of[2], 1), 0, 1)
    first_kernel = gaussian(streams_of[3], (3, 3, C, C), (9 * C) ** -0.5, 0.1875)
    first_bias = gaussian(streams_of[4], (C,), 0.5, 3.0, (), jnp.float32)
    second_kernel = gaussian(streams_of[5], (3, 3, C, C), (9 * C) ** -0.5, 0.1875)
    second_bias = gaussian(streams_of[6], (C,), 0.5, 3.0, (), jnp.float32)
    return dict(pair_features=pair_features, out_grad=out_grad, bin_valid=bin_valid, first_kernel=first_kernel, first_bias=first_bias, second_kernel=second_kernel, second_bias=second_bias)


def tap_total_sum(sliding_window, kernel, dilation, anchor, out_rows, out_cols, flipped):
    channels = sliding_window.shape[-1]
    slot_count = sliding_window.shape[0]
    facing = -1 if flipped else 1
    running = jnp.zeros((slot_count * out_rows * out_cols, kernel.shape[-1]), jnp.float32)
    for row_tap in range(3):
        for col_tap in range(3):
            row_from = anchor + facing * (row_tap - 1) * dilation
            col_from = anchor + facing * (col_tap - 1) * dilation
            shifted = sliding_window[:, row_from:row_from + out_rows, col_from:col_from + out_cols, :].reshape(-1, channels)
            if flipped:
                running = running + lax.dot_general(shifted, kernel[row_tap, col_tap], (((1,), (1,)), ((), ())), preferred_element_type=jnp.float32)
            else:
                running = running + jnp.dot(shifted, kernel[row_tap, col_tap], preferred_element_type=jnp.float32)
    return running.reshape(slot_count, out_rows, out_cols, kernel.shape[-1])

def kernel_gradient(local_values, sliding_window, dilation, anchor):
    channels = local_values.shape[-1]
    out_rows = local_values.shape[1]
    out_cols = local_values.shape[2]
    flat_local = local_values.reshape(-1, channels)
    tap_grid = []
    for row_tap in range(3):
        tap_line = []
        for col_tap in range(3):
            row_from = anchor - (row_tap - 1) * dilation
            col_from = anchor - (col_tap - 1) * dilation
            shifted = sliding_window[:, row_from:row_from + out_rows, col_from:col_from + out_cols, :].reshape(-1, sliding_window.shape[-1])
            tap_line.append(lax.dot_general(flat_local, shifted, (((0,), (0,)), ((), ())), preferred_element_type=jnp.float32))
        tap_grid.append(jnp.stack(tap_line))
    return jnp.stack(tap_grid)

def neighbour_patch(band_array, band_tile_block, rim_width):
    tile_row = band_tile_block // BAND_DIAGONALS
    diagonal = band_tile_block % BAND_DIAGONALS
    row_blocks = []
    for row_step in (-1, 0, 1):
        col_blocks = []
        for col_step in (-1, 0, 1):
            other_row = tile_row + row_step
            other_diag = diagonal + col_step - row_step
            present = (other_row >= 0) & (other_row < TILE_ROWS) & (other_diag >= 0) & (other_diag < BAND_DIAGONALS)
            other_tile = jnp.clip(other_row * BAND_DIAGONALS + other_diag, 0, TILES - 1).astype(jnp.int32)
            neighbour = band_array[other_tile]
            col_blocks.append(jnp.where(present, neighbour, jnp.zeros((), band_array.dtype)))
        row_blocks.append(jnp.concatenate(col_blocks, axis=1))
    assembled = jnp.concatenate(row_blocks, axis=0)
    return assembled[TILE_BINS - rim_width:2 * TILE_BINS + rim_width, TILE_BINS - rim_width:2 * TILE_BINS + rim_width][None]

def reference(pair_features, out_grad, bin_valid, first_kernel, first_bias, second_kernel, second_bias):
    band_index = np.arange(TILES)
    linear_of_tile = (band_index - BAND_DIAGONALS) % TILES
    band_order = linear_of_tile % N_TILE * TPG + linear_of_tile // N_TILE
    position_order = (band_index % TPG * N_TILE + band_index // TPG + BAND_DIAGONALS) % TILES
    first_row = band_index // BAND_DIAGONALS * TILE_BINS
    first_col = (band_index // BAND_DIAGONALS + band_index % BAND_DIAGONALS) * TILE_BINS
    row_pos = jnp.asarray(first_row[:, None] + np.arange(TILE_BINS)[None, :], dtype=jnp.int32)
    col_pos = jnp.asarray(first_col[:, None] + np.arange(TILE_BINS)[None, :], dtype=jnp.int32)
    diagonal_distance = col_pos[:, None, :] - row_pos[:, :, None]
    valid_row_mask = bin_valid[row_pos] > 0
    valid_column_mask = bin_valid[col_pos] > 0
    live_cell_mask = ((diagonal_distance >= FIRST_DILATION + SECOND_DILATION) & (diagonal_distance <= (BAND_DIAGONALS - 1) * TILE_BINS - FIRST_DILATION - SECOND_DILATION) & valid_row_mask[:, :, None] & valid_column_mask[:, None, :]).astype(jnp.float32)
    live_wide = live_cell_mask[..., None]
    live_features = pair_features[band_order] * live_wide.astype(jnp.bfloat16)
    tile_ids = jnp.arange(TILES, dtype=jnp.int32)

    def first_conv(band_tile_block):
        sliding_window = neighbour_patch(live_features, band_tile_block, FIRST_DILATION)
        return tap_total_sum(sliding_window, first_kernel, FIRST_DILATION, FIRST_DILATION, TILE_BINS, TILE_BINS, False)[0] + first_bias
    pre_one = lax.map(first_conv, tile_ids)
    hidden_state = (jax.nn.silu(pre_one) * live_wide).astype(jnp.bfloat16)

    def second_conv(band_tile_block):
        sliding_window = neighbour_patch(hidden_state, band_tile_block, SECOND_DILATION)
        return tap_total_sum(sliding_window, second_kernel, SECOND_DILATION, SECOND_DILATION, TILE_BINS, TILE_BINS, False)[0] + second_bias
    pre_two = lax.map(second_conv, tile_ids)
    block_out = (live_features.astype(jnp.float32) + live_wide * pre_two).astype(jnp.bfloat16)
    second_gradient = out_grad[band_order] * live_wide.astype(jnp.bfloat16)

    def back_two(kernel_total_sum, band_tile_block):
        sliding_window = neighbour_patch(second_gradient, band_tile_block, SECOND_DILATION)
        kernel_total_sum = kernel_total_sum + kernel_gradient(hidden_state[band_tile_block][None], sliding_window, SECOND_DILATION, SECOND_DILATION)
        hidden_gradient = tap_total_sum(sliding_window, second_kernel, SECOND_DILATION, SECOND_DILATION, TILE_BINS, TILE_BINS, True)[0]
        pre_act = pre_one[band_tile_block]
        logistic = jax.nn.sigmoid(pre_act)
        silu_slope = logistic * (1.0 + pre_act * (1.0 - logistic))
        first_gradient = (hidden_gradient * live_wide[band_tile_block] * silu_slope).astype(jnp.bfloat16)
        return (kernel_total_sum, first_gradient)
    kernel_two_sum, first_gradient = lax.scan(back_two, jnp.zeros((3, 3, C, C), jnp.float32), tile_ids)
    ordered_grad = out_grad[band_order]

    def back_one(kernel_total_sum, band_tile_block):
        sliding_window = neighbour_patch(first_gradient, band_tile_block, FIRST_DILATION)
        kernel_total_sum = kernel_total_sum + kernel_gradient(live_features[band_tile_block][None], sliding_window, FIRST_DILATION, FIRST_DILATION)
        returned_values = tap_total_sum(sliding_window, first_kernel, FIRST_DILATION, FIRST_DILATION, TILE_BINS, TILE_BINS, True)[0]
        grad_tile = (live_wide[band_tile_block] * (ordered_grad[band_tile_block].astype(jnp.float32) + returned_values)).astype(jnp.bfloat16)
        return (kernel_total_sum, grad_tile)
    kernel_one_sum, feature_grad = lax.scan(back_one, jnp.zeros((3, 3, C, C), jnp.float32), tile_ids)
    grad_scale = 1.0 / math.sqrt(TILES * TILE_BINS * TILE_BINS)
    bias_one_grad = lax.optimization_barrier(jnp.sum(first_gradient.astype(jnp.float32), axis=(0, 1, 2))) * grad_scale
    bias_two_grad = lax.optimization_barrier(jnp.sum(second_gradient.astype(jnp.float32), axis=(0, 1, 2))) * grad_scale
    return (block_out[position_order], feature_grad[position_order], kernel_one_sum * grad_scale, bias_one_grad, kernel_two_sum * grad_scale, bias_two_grad)
```

```python
import math

import jax
import jax.numpy as jnp
import numpy as np
from jax import lax
from jax.sharding import PartitionSpec as P

FIRST_DILATION = 8
SECOND_DILATION = 16
BAND_DIAGONALS = 4
AXES = ("tile", "sub")


def routes(groups, subs):
    rows = groups // BAND_DIAGONALS

    def device(band_tile, sub):
        return (band_tile - BAND_DIAGONALS) % groups * subs + sub

    above, below, left, right = [], [], [], []
    for k in range(groups):
        i, j = divmod(k, BAND_DIAGONALS)
        for s in range(subs):
            me = device(k, s)
            if s > 0:
                above.append((device(k, s - 1), me))
            elif i > 0 and j < BAND_DIAGONALS - 1:
                above.append((device(k - BAND_DIAGONALS + 1, subs - 1), me))
            if s < subs - 1:
                below.append((device(k, s + 1), me))
            elif i < rows - 1 and j > 0:
                below.append((device(k + BAND_DIAGONALS - 1, 0), me))
            if j > 0:
                left.append((device(k - 1, s), me))
            if j < BAND_DIAGONALS - 1:
                right.append((device(k + 1, s), me))
    return above, below, left, right


def taps(window, kernel, dilation, out_rows, out_cols, flipped):
    channels = window.shape[-1]
    facing = -1 if flipped else 1
    running = None
    for row_tap in range(3):
        for col_tap in range(3):
            row_from = dilation + facing * (row_tap - 1) * dilation
            col_from = dilation + facing * (col_tap - 1) * dilation
            shifted = window[
                row_from : row_from + out_rows, col_from : col_from + out_cols, :
            ].reshape(-1, channels)
            dims = (((1,), (1 if flipped else 0,)), ((), ()))
            part = lax.dot_general(
                shifted, kernel[row_tap, col_tap], dims, preferred_element_type=jnp.float32
            )
            running = part if running is None else running + part
    return running.reshape(out_rows, out_cols, channels)


def kernel_terms(inputs, grads, dilation, window_is_input):
    rows, cols, channels = (grads if window_is_input else inputs).shape
    lines = []
    for row_tap in range(3):
        for col_tap in range(3):
            sign = 1 if window_is_input else -1
            row_from = dilation + sign * (row_tap - 1) * dilation
            col_from = dilation + sign * (col_tap - 1) * dilation
            window = inputs if window_is_input else grads
            shifted = window[row_from : row_from + rows, col_from : col_from + cols].reshape(
                -1, channels
            )
            pair = (
                (shifted, grads.reshape(-1, channels))
                if window_is_input
                else (inputs.reshape(-1, channels), shifted)
            )
            lines.append(
                lax.dot_general(
                    *pair, (((0,), (0,)), ((), ())), preferred_element_type=jnp.float32
                )
            )
    return jnp.concatenate(lines, axis=0)


def all_sum(terms, groups, subs):
    stages = []
    step = 1
    while step < groups:
        stages.append(("tile", step, groups))
        step *= 2
    step = 1
    while step < subs:
        stages.append(("sub", step, subs))
        step *= 2
    held = terms
    for axis, step, size in stages:
        half = held.shape[0] // 2
        upper = (lax.axis_index(axis) // step) % 2 == 1
        low, high = held[:half], held[half:]
        away = jnp.where(upper, low, high).astype(jnp.bfloat16)
        mine = jnp.where(upper, high, low)
        came = lax.ppermute(away, axis, [(i, i ^ step) for i in range(size)])
        held = mine + came.astype(jnp.float32)
    held = held.astype(jnp.bfloat16)
    for axis, step, size in reversed(stages):
        upper = (lax.axis_index(axis) // step) % 2 == 1
        came = lax.ppermute(held, axis, [(i, i ^ step) for i in range(size)])
        held = jnp.concatenate(
            [jnp.where(upper, came, held), jnp.where(upper, held, came)], axis=0
        )
    return held.astype(jnp.float32)


def on_device(
    pair_features, out_grad, bin_valid, first_kernel, first_bias, second_kernel, second_bias
):
    slots, strip, side, channels = pair_features.shape
    groups = lax.axis_size("tile")
    subs = lax.axis_size("sub")
    assert slots == 1
    group = lax.axis_index("tile")
    sub = lax.axis_index("sub")
    band_tile = (group + BAND_DIAGONALS) % groups
    tile_row = band_tile // BAND_DIAGONALS
    tile_col = tile_row + band_tile % BAND_DIAGONALS
    map_rows = groups // BAND_DIAGONALS * side
    above, below, left, right = routes(groups, subs)
    features = pair_features[0]
    cotangent = out_grad[0]

    def widened(values, rim):
        from_above = lax.ppermute(values[strip - rim :], AXES, above)
        from_below = lax.ppermute(values[:rim], AXES, below)
        tall = jnp.concatenate([from_above, values, from_below], axis=0)
        from_left = lax.ppermute(tall[:, side - rim :], AXES, left)
        from_right = lax.ppermute(tall[:, :rim], AXES, right)
        return jnp.concatenate([from_left, tall, from_right], axis=1)

    rim = SECOND_DILATION
    row_pos = tile_row * side + sub * strip - rim + jnp.arange(strip + 2 * rim, dtype=jnp.int32)
    col_pos = tile_col * side - rim + jnp.arange(side + 2 * rim, dtype=jnp.int32)
    padded_valid = jnp.pad(bin_valid, (rim, rim))
    row_ok = (
        (lax.dynamic_slice_in_dim(padded_valid, row_pos[0] + rim, strip + 2 * rim) > 0)
        & (row_pos >= 0)
        & (row_pos < map_rows)
    )
    col_ok = lax.dynamic_slice_in_dim(padded_valid, col_pos[0] + rim, side + 2 * rim) > 0
    distance = col_pos[None, :] - row_pos[:, None]
    live_wide = (
        row_ok[:, None]
        & col_ok[None, :]
        & (distance >= FIRST_DILATION + SECOND_DILATION)
        & (distance <= (BAND_DIAGONALS - 1) * side - FIRST_DILATION - SECOND_DILATION)
    )[..., None]

    def live_at(width):
        cut = rim - width
        return live_wide[cut : strip + 2 * rim - cut, cut : side + 2 * rim - cut]

    own_live = live_at(0).astype(jnp.float32)
    live16 = live_at(FIRST_DILATION).astype(jnp.bfloat16)
    feature_patch = widened(features, FIRST_DILATION) * live16
    grad_patch = widened(cotangent, SECOND_DILATION) * live_wide.astype(jnp.bfloat16)
    d1, d2 = FIRST_DILATION, SECOND_DILATION
    live_features = feature_patch[d1 : d1 + strip, d1 : d1 + side]
    second_gradient = grad_patch[d2 : d2 + strip, d2 : d2 + side]
    pre_one = taps(feature_patch, first_kernel, d1, strip, side, False) + first_bias
    logistic = jax.nn.sigmoid(pre_one)
    hidden = (pre_one * logistic * own_live).astype(jnp.bfloat16)
    hidden_patch = widened(hidden, d2)
    hidden_gradient = taps(grad_patch, second_kernel, d2, strip, side, True)
    slope = logistic * (1.0 + pre_one * (1.0 - logistic))
    first_gradient = (hidden_gradient * own_live * slope).astype(jnp.bfloat16)
    first_patch = widened(first_gradient, d1)
    one_terms = kernel_terms(feature_patch, first_gradient, d1, True)
    two_terms = kernel_terms(hidden, grad_patch, d2, False)
    bias_one = jnp.sum(first_gradient.astype(jnp.float32), axis=(0, 1))
    bias_two = jnp.sum(second_gradient.astype(jnp.float32), axis=(0, 1))
    count = one_terms.shape[0]
    unit = groups * subs * 16
    spare = -(2 * count + 2) % unit
    terms = jnp.concatenate(
        [
            one_terms,
            two_terms,
            bias_one[None],
            bias_two[None],
            jnp.zeros((spare, channels), jnp.float32),
        ],
        axis=0,
    )
    sums = all_sum(terms, groups, subs) * (1.0 / math.sqrt(groups * side * side))
    pre_two = taps(hidden_patch, second_kernel, d2, strip, side, False) + second_bias
    block_out = (live_features.astype(jnp.float32) + own_live * pre_two).astype(jnp.bfloat16)
    returned = taps(first_patch, first_kernel, d1, strip, side, True)
    feature_grad = (own_live * (cotangent.astype(jnp.float32) + returned)).astype(jnp.bfloat16)
    shape = first_kernel.shape
    return (
        block_out[None],
        feature_grad[None],
        sums[:count].reshape(shape),
        sums[2 * count],
        sums[count : 2 * count].reshape(shape),
        sums[2 * count + 1],
    )


def solution(mesh):
    in_specs = (P("tile", "sub", None, None), P("tile", "sub", None, None), P(), P(), P(), P(), P())
    out_specs = (P("tile", "sub", None, None), P("tile", "sub", None, None), P(), P(), P(), P())
    return jax.shard_map(
        on_device, mesh=mesh, in_specs=in_specs, out_specs=out_specs, check_vma=False
    )
```

```python
import functools
import math

import jax
import jax.numpy as jnp
from jax import lax
from jax.experimental import pallas as pl
from jax.experimental.pallas import tpu as pltpu
from jax.sharding import PartitionSpec as P

FIRST_DILATION = 8
SECOND_DILATION = 16
BAND_DIAGONALS = 4
AXES = ("tile", "sub")
BLOCK_ROWS = 8
GRAD_ROWS = 4
VMEM = pltpu.MemorySpace.VMEM
SMEM = pltpu.MemorySpace.SMEM


def routes(groups, subs):
    rows = groups // BAND_DIAGONALS

    def device(band_tile, sub):
        return (band_tile - BAND_DIAGONALS) % groups * subs + sub

    above, below, left, right = [], [], [], []
    for k in range(groups):
        i, j = divmod(k, BAND_DIAGONALS)
        for s in range(subs):
            me = device(k, s)
            if s > 0:
                above.append((device(k, s - 1), me))
            elif i > 0 and j < BAND_DIAGONALS - 1:
                above.append((device(k - BAND_DIAGONALS + 1, subs - 1), me))
            if s < subs - 1:
                below.append((device(k, s + 1), me))
            elif i < rows - 1 and j > 0:
                below.append((device(k + BAND_DIAGONALS - 1, 0), me))
            if j > 0:
                left.append((device(k - 1, s), me))
            if j < BAND_DIAGONALS - 1:
                right.append((device(k + 1, s), me))
    return above, below, left, right


def live_mask(bounds, cols, row, first, count):
    at = cols[pl.ds(first, count), :]
    return (at >= bounds[0, row]) & (at <= bounds[1, row])


def cut(values, keep):
    return values * jnp.where(keep, 1.0, 0.0).astype(values.dtype)


def fill_window(window, pieces, bounds, cols, rim):
    above, own, below, left, right = pieces
    strip, side, _ = own.shape
    skip = SECOND_DILATION - rim

    def centre(source, offset, count):
        def body(r, carry):
            row = r + offset
            keep = live_mask(bounds, cols, row + skip, SECOND_DILATION, side)
            window[row, pl.ds(rim, side), :] = cut(source[r], keep)
            return carry

        lax.fori_loop(0, count, body, 0)

    centre(above, 0, rim)
    centre(own, rim, strip)
    centre(below, rim + strip, rim)

    def edges(row, carry):
        keep = live_mask(bounds, cols, row + skip, skip, rim)
        window[row, pl.ds(0, rim), :] = cut(left[row], keep)
        keep = live_mask(bounds, cols, row + skip, SECOND_DILATION + side, rim)
        window[row, pl.ds(rim + side, rim), :] = cut(right[row], keep)
        return carry

    lax.fori_loop(0, strip + 2 * rim, edges, 0)


def convolve(window, weights, rim, strip, side, finish):
    channels = window.shape[-1]
    block = min(BLOCK_ROWS, rim)

    def body(step, carry):
        base = step // (rim // block) * (2 * rim) + step % (rim // block) * block
        parts = [
            window[pl.ds(base + v * rim, block), pl.ds(w * rim, side), :].reshape(
                block * side, channels
            )
            for v in range(4)
            for w in range(3)
        ]
        out = jnp.dot(
            jnp.concatenate(parts, axis=1), weights[...], preferred_element_type=jnp.float32
        )
        for half in range(2):
            for r in range(block):
                finish(
                    base + half * rim + r,
                    out[r * side : (r + 1) * side, half * channels : (half + 1) * channels],
                )
        return carry

    lax.fori_loop(0, strip // (2 * block), body, 0)


def own_mask(bounds, cols, row, side):
    return live_mask(bounds, cols, row + SECOND_DILATION, SECOND_DILATION, side)


def fold(values):
    rows, channels = values.shape
    return jnp.sum(values.reshape(rows // 8, 8, channels), axis=0)


def hidden_kernel(
    bounds, cols, above, own, below, left, right, weights, bias, hidden, slope, window
):
    strip, side, _ = own.shape
    fill_window(window, (above, own, below, left, right), bounds, cols, FIRST_DILATION)

    def finish(row, sums):
        keep = own_mask(bounds, cols, row, side)
        pre = sums + bias[...]
        gate = jax.nn.sigmoid(pre)
        hidden[row] = jnp.where(keep, pre * gate, 0.0).astype(hidden.dtype)
        slope[row] = jnp.where(keep, gate * (1.0 + pre * (1.0 - gate)), 0.0)

    convolve(window, weights, FIRST_DILATION, strip, side, finish)


def gradient_kernel(
    bounds, cols, above, own, below, left, right, weights, slope, grad, biases, window
):
    strip, side, _ = own.shape
    rim = SECOND_DILATION
    fill_window(window, (above, own, below, left, right), bounds, cols, rim)
    biases[...] = jnp.zeros_like(biases)

    def finish(row, sums):
        value = (sums * slope[row]).astype(grad.dtype)
        grad[row] = value
        biases[0] += fold(value.astype(jnp.float32))
        biases[1] += fold(window[row + rim, pl.ds(rim, side), :].astype(jnp.float32))

    convolve(window, weights, rim, strip, side, finish)


def terms_kernel(features, first_grad, hidden, second_grad, terms, sum_one, sum_two):
    strip, side, channels = first_grad.shape
    rows = GRAD_ROWS

    def pairs(local, window, rim, order, total, base):
        flat = local[pl.ds(base, rows)].reshape(rows * side, channels)
        parts = [
            window[pl.ds(base + u * rim, rows), pl.ds(w * rim, side), :].reshape(
                rows * side, channels
            )
            for u in order
            for w in order
        ]
        total[...] += lax.dot_general(
            flat,
            jnp.concatenate(parts, axis=1),
            (((0,), (0,)), ((), ())),
            preferred_element_type=jnp.float32,
        )

    sum_one[...] = jnp.zeros_like(sum_one)
    sum_two[...] = jnp.zeros_like(sum_two)

    def body(step, carry):
        base = step * rows
        pairs(first_grad, features, FIRST_DILATION, (0, 1, 2), sum_one, base)
        pairs(hidden, second_grad, SECOND_DILATION, (2, 1, 0), sum_two, base)
        return carry

    lax.fori_loop(0, strip // rows, body, 0)
    for tap in range(9):
        at = pl.ds(tap * channels, channels)
        terms[at, :] = sum_one[:, at].T
        terms[pl.ds((9 + tap) * channels, channels), :] = sum_two[:, at]


def output_kernel(
    rim, bounds, cols, above, own, below, left, right, weights, bias, raw, result, window
):
    strip, side, _ = own.shape
    fill_window(window, (above, own, below, left, right), bounds, cols, rim)

    def finish(row, sums):
        keep = own_mask(bounds, cols, row, side)
        value = raw[row].astype(jnp.float32) + (sums + bias[...])
        result[row] = jnp.where(keep, value, 0.0).astype(result.dtype)

    convolve(window, weights, rim, strip, side, finish)


def call(body, name, args, outs, scratch=(), smem=1):
    specs = [
        pl.BlockSpec(memory_space=SMEM if i < smem else VMEM) for i in range(len(args))
    ]
    return pl.pallas_call(
        body,
        out_shape=[jax.ShapeDtypeStruct(*o) for o in outs],
        in_specs=specs,
        out_specs=[pl.BlockSpec(memory_space=VMEM) for _ in outs],
        scratch_shapes=[pltpu.VMEM(*s) for s in scratch],
        name=name,
    )(*args)


def paired_weights(kernel, flipped):
    if flipped:
        kernel = jnp.flip(kernel, (0, 1)).swapaxes(2, 3)
    none = jnp.zeros_like(kernel[:1])
    pair = jnp.concatenate(
        [jnp.concatenate([kernel, none], axis=0), jnp.concatenate([none, kernel], axis=0)], axis=3
    )
    return pair.reshape(-1, pair.shape[-1])


def radices(size):
    plan, stride = [], 1
    if size % 4 and size % 2 == 0 or size == 8:
        plan.append((2, 1))
        stride = 2
    while stride < size:
        radix = 4 if size // stride % 4 == 0 else 2
        plan.append((radix, stride))
        stride *= radix
    return plan


def all_sum(terms, extras, groups, subs):
    bf16, f32 = jnp.bfloat16, jnp.float32
    devices = groups * subs
    width = terms.shape[-1]
    few = extras.shape[0]
    held = terms.reshape(devices, -1, width)
    tail = jnp.concatenate(
        [extras[None], jnp.zeros((devices - 1, few, width), f32)], axis=0
    )
    stages = [("tile", r, t, groups) for r, t in radices(groups)]
    stages += [("sub", r, t, subs) for r, t in radices(subs)]

    def wire(body, end):
        high = lax.reduce_precision(end, 8, 7)
        return jnp.concatenate([body, high, end - high], axis=-2).astype(bf16)

    def unwire(came):
        body = came[..., : -2 * few, :]
        return body, came[..., -2 * few : -few, :].astype(f32) + came[..., -few:, :].astype(f32)

    def trade(value, axis, radix, stride, size, shift):
        def partner(i):
            digit = i // stride % radix
            return i + ((digit + shift) % radix - digit) * stride

        return lax.ppermute(value, axis, [(i, partner(i)) for i in range(size)])

    for axis, radix, stride, size in stages:
        digit = lax.axis_index(axis) // stride % radix
        held = held.reshape(radix, -1, *held.shape[-2:])
        tail = tail.reshape(radix, -1, *tail.shape[-2:])

        def part(which):
            return (
                lax.dynamic_index_in_dim(held, which % radix, keepdims=False),
                lax.dynamic_index_in_dim(tail, which % radix, keepdims=False),
            )

        arrived = [
            trade(wire(*part(digit + shift)), axis, radix, stride, size, shift)
            for shift in range(1, radix)
        ]
        held, tail = part(digit)
        for came in arrived:
            body, end = unwire(came)
            held = held + body.astype(f32)
            tail = tail + end
    sent = wire(held, tail)
    for axis, radix, stride, size in reversed(stages):
        digit = lax.axis_index(axis) // stride % radix
        parts = [sent] + [trade(sent, axis, radix, stride, size, s) for s in range(1, radix)]
        if radix == 2:
            first, second = (jnp.where(digit == 0, parts[i], parts[1 - i]) for i in (0, 1))
            sent = jnp.concatenate([first, second], axis=0)
        else:
            sent = jnp.zeros((radix, *parts[0].shape), bf16)
            for shift, value in enumerate(parts):
                sent = lax.dynamic_update_index_in_dim(sent, value, (digit - shift) % radix, 0)
            sent = sent.reshape(-1, *sent.shape[-2:])
    body, end = unwire(sent)
    return body.reshape(-1, width).astype(f32), end[0]


def on_device(
    pair_features, out_grad, bin_valid, first_kernel, first_bias, second_kernel, second_bias
):
    slots, strip, side, channels = pair_features.shape
    groups = lax.axis_size("tile")
    subs = lax.axis_size("sub")
    assert slots == 1 and strip % (2 * SECOND_DILATION) == 0
    group = lax.axis_index("tile")
    sub = lax.axis_index("sub")
    band_tile = (group + BAND_DIAGONALS) % groups
    tile_row = band_tile // BAND_DIAGONALS
    tile_col = tile_row + band_tile % BAND_DIAGONALS
    map_rows = groups // BAND_DIAGONALS * side
    above, below, left, right = routes(groups, subs)
    features = pair_features[0]
    cotangent = out_grad[0]
    d1, d2 = FIRST_DILATION, SECOND_DILATION
    bf16, f32 = jnp.bfloat16, jnp.float32

    def rows_of(values, rim):
        return (
            lax.ppermute(values[strip - rim :], AXES, above),
            lax.ppermute(values[:rim], AXES, below),
        )

    def pieces_of(values, rim):
        upper, lower = rows_of(values, rim)

        def edge(first):
            return jnp.concatenate(
                [part[:, first : first + rim] for part in (upper, values, lower)], axis=0
            )

        from_left = lax.ppermute(edge(side - rim), AXES, left)
        from_right = lax.ppermute(edge(0), AXES, right)
        return upper, values, lower, from_left, from_right

    row_pos = tile_row * side + sub * strip - d2 + jnp.arange(strip + 2 * d2, dtype=jnp.int32)
    padded = jnp.pad(bin_valid, (d2, d2))
    first_row = tile_row * side + sub * strip
    first_col = tile_col * side
    row_ok = (
        (lax.dynamic_slice_in_dim(padded, first_row, strip + 2 * d2) > 0)
        & (row_pos >= 0)
        & (row_pos < map_rows)
    )
    col_ok = lax.dynamic_slice_in_dim(padded, first_col, side + 2 * d2) > 0
    least = row_pos + (d1 + d2) - first_col
    most = row_pos + ((BAND_DIAGONALS - 1) * side - d1 - d2) - first_col
    far = jnp.int32(1 << 20)
    bounds = jnp.stack([jnp.where(row_ok, least, far), most])
    col_pos = jnp.arange(side + 2 * d2, dtype=jnp.int32) - d2
    cols = jnp.broadcast_to(
        jnp.where(col_ok, col_pos, -far)[:, None], (side + 2 * d2, channels)
    )

    feature_pieces = pieces_of(features, d1)
    grad_pieces = pieces_of(cotangent, d2)
    one_forward = paired_weights(first_kernel, False)
    two_forward = paired_weights(second_kernel, False)
    one_back = paired_weights(first_kernel, True)
    two_back = paired_weights(second_kernel, True)
    tile_shape = (strip, side, channels)
    window_one = (strip + 2 * d1, side + 2 * d1, channels)
    window_two = (strip + 2 * d2, side + 2 * d2, channels)

    hidden, slope, feature_window = call(
        hidden_kernel,
        "hidden",
        (bounds, cols, *feature_pieces, one_forward, first_bias[None]),
        [(tile_shape, bf16), (tile_shape, f32), (window_one, bf16)],
    )
    hidden_pieces = pieces_of(hidden, d2)
    first_grad, biases, grad_window = call(
        gradient_kernel,
        "gradient",
        (bounds, cols, *grad_pieces, two_back, slope),
        [(tile_shape, bf16), ((2, 8, channels), f32), (window_two, bf16)],
    )
    first_pieces = pieces_of(first_grad, d1)
    count = 9 * channels
    (terms,) = call(
        terms_kernel,
        "terms",
        (feature_window, first_grad, hidden, grad_window),
        [((2 * count, channels), f32)],
        [((channels, count), f32), ((channels, count), f32)],
        smem=0,
    )
    extras = jnp.pad(jnp.sum(biases, axis=1), ((0, 2), (0, 0)))
    scale = 1.0 / math.sqrt(groups * side * side)
    sums, bias_sums = all_sum(terms, extras, groups, subs)
    sums, bias_sums = sums * scale, bias_sums * scale
    (block_out,) = call(
        functools.partial(output_kernel, d2),
        "block",
        (bounds, cols, *hidden_pieces, two_forward, second_bias[None], features),
        [(tile_shape, bf16)],
        [(window_two, bf16)],
    )
    (feature_grad,) = call(
        functools.partial(output_kernel, d1),
        "returned",
        (bounds, cols, *first_pieces, one_back, jnp.zeros((1, channels), f32), cotangent),
        [(tile_shape, bf16)],
        [(window_one, bf16)],
    )
    shape = first_kernel.shape
    return (
        block_out[None],
        feature_grad[None],
        sums[:count].reshape(shape),
        bias_sums[0],
        sums[count:].reshape(shape),
        bias_sums[1],
    )


def solution(mesh):
    in_specs = (P("tile", "sub", None, None), P("tile", "sub", None, None), P(), P(), P(), P(), P())
    out_specs = (P("tile", "sub", None, None), P("tile", "sub", None, None), P(), P(), P(), P())
    return jax.shard_map(
        on_device, mesh=mesh, in_specs=in_specs, out_specs=out_specs, check_vma=False
    )
```
